256 devices in a mesh: section: 8 (over z), col: 32 (over y, x, core).
Axes of the slice: x: 4, y: 4, z: 8, core: 2. Of those that a mesh axis runs over, the one named last changes fastest.
Arguments:
- tiles: bfloat16 [1024, 12, 128, 128], P('col', None, 'section'), may hold values from 0.0099487305 to 1
- offsets: int32 [1024, 12], replicated, may hold values from -6 to 6, as said below
- counts: int32 [1024], replicated, may hold values from 1 to 12
- ranks: int32 [1024, 25, 128, 128], P('col', None, 'section'), may hold values from 0 to 3199, as said below
Outputs:
- pruned: bfloat16 [1024, 25, 128, 128], P('col', None, 'section')
The draws below stay inside these ranges and needn't reach their ends.
Inputs may be any that keep to these rules, and one draw needn't show every extreme that they name: Within each panel the 12 offsets are distinct, each from -6 to 6. For every panel j and column c, ranks[j, :, c, :] holds each of 0 .. 3199 once.
All inputs are finite; a program needn't handle non-finite values.
Results may differ from the reference program's by a relative error of at most 0.001.
Values may be sent and summed in bfloat16 or wider, within the bound.
A program may use at most 128 MiB of HBM per device.

```python
import math
import jax
import jax.numpy as jnp
from jax import lax

TILE = 128
KB = 12
W = 6
TOPK = 256
NB = 1024
OB = 25


def draw_offsets(key, part):
    keys = jax.random.split(key, NB)
    perms = jax.vmap(lambda single: jax.random.permutation(single, 2 * W + 1))(keys)
    return (perms[:, :KB] - W).astype(jnp.int32)


def draw_ranks(key, part):
    keys = jax.random.split(key, NB * TILE)
    perms = jax.vmap(lambda single: jax.random.permutation(single, OB * TILE))(keys)
    return perms.reshape(NB, TILE, OB, TILE).transpose(0, 2, 1, 3).astype(jnp.int32)


def place_ends(array, rng, least, largest):
    longest = array.shape.index(max(array.shape))
    spots = []
    for shift in (0, 1):
        where = [jax.random.randint(jax.random.fold_in(rng, axis), (), 0, length) for axis, length in enumerate(array.shape)]
        where[longest] = (where[longest] + shift) % array.shape[longest]
        spots.append(tuple(where))
    return array.at[spots[0]].set(least).at[spots[1]].set(largest)


def levels(stream_key, shape, pieces, least, high):
    def one(position, shards_of):
        heights = jax.random.uniform(jax.random.fold_in(jax.random.fold_in(stream_key, 6), position), (shards_of,), jnp.float32, least / len(pieces), high / len(pieces))
        return jnp.repeat(jnp.exp(heights), shape[position] // shards_of).reshape((-1,) + (1,) * (len(shape) - position - 1))

    factor_of = one(*pieces[0])
    for cut in pieces[1:]:
        factor_of = factor_of * one(*cut)
    return factor_of


def setup_inputs(seed: int = 0) -> dict:
    key_of = jax.random.split(jax.random.key(seed), 5)
    tiles = jnp.clip(jnp.exp(math.log(1.0) - 4.61031033 * jax.random.uniform(key_of[0], (NB, KB, TILE, TILE), jnp.float32) ** levels(key_of[0], (NB, KB, TILE, TILE), ((0, 32), (2, 8)), -0.2, 0.2)), 0.0099487305, 1.0).astype(jnp.bfloat16)
    offsets = draw_offsets(jax.random.fold_in(key_of[4], 71), 0)
    counts = place_ends(jax.random.randint(key_of[2], (NB,), 1, KB + 1), jax.random.fold_in(key_of[2], 1), 1, KB).astype(jnp.int32)
    ranks = draw_ranks(jax.random.fold_in(key_of[4], 71), 0)
    return {"tiles": tiles, "offsets": offsets, "counts": counts, "ranks": ranks}


def reference(tiles, offsets, counts, ranks):
    total = tiles.shape[0]
    slots = tiles.shape[1]
    bands = 4 * W + 1
    padded = jnp.pad(tiles, ((W, W), (0, 0), (0, 0), (0, 0)))
    pad_off = jnp.pad(offsets, ((W, W), (0, 0)))
    pad_cnt = jnp.pad(counts, ((W, W),))
    slot_ids = jnp.arange(slots, dtype=jnp.int32)

    def one_panel(panel):
        own = lax.dynamic_index_in_dim(tiles, panel, 0, False).astype(jnp.float32)
        own_off = lax.dynamic_index_in_dim(offsets, panel, 0, False)
        own_cnt = lax.dynamic_index_in_dim(counts, panel, 0, False)
        where_at = (panel + W + own_off).astype(jnp.int32)
        firsts = padded[where_at].astype(jnp.float32)
        first_off = pad_off[where_at]
        first_cnt = pad_cnt[where_at]
        row_own = panel + own_off
        ok_own = (slot_ids < own_cnt) & (row_own >= 0) & (row_own < total)
        row_first = row_own[:, None] + first_off
        ok_first = (slot_ids[None, :] < first_cnt[:, None]) & (row_first >= 0) & (row_first < total)
        weight = (ok_own[:, None] & ok_first).astype(jnp.float32)
        target = own_off[:, None] + first_off + 2 * W
        place = (jnp.arange(bands, dtype=jnp.int32)[:, None, None] == target[None]).astype(jnp.float32) * weight[None]
        products = jnp.einsum('kcx,klxr->klcr', own, firsts, precision=lax.Precision.HIGHEST)
        expanded = jnp.einsum('okl,klcr->ocr', place, products, precision=lax.Precision.HIGHEST)
        keep = lax.dynamic_index_in_dim(ranks, panel, 0, False) < TOPK
        squared = jnp.where(keep, expanded * expanded, jnp.float32(0.0))
        totals = jnp.sum(squared, axis=(0, 2), keepdims=True)
        return (TOPK * squared / (totals + 1e-6)).astype(jnp.bfloat16)

    return lax.map(one_panel, jnp.arange(total, dtype=jnp.int32))
```

```python
import functools

import jax
import jax.numpy as jnp
from jax import lax
from jax.experimental import pallas as pl
from jax.experimental.pallas import tpu as pltpu
from jax.sharding import PartitionSpec as P

W = 6
TOPK = 256
GROUP = 4
MESH = pl.DeviceIdType.MESH


def list_rank(panels):
    return [m if m < W else (m - panels + 2 * W if m >= panels - W else m + W) for m in range(panels)]


def pack_kernel(panels, slots, first_ref, tiles_ref, out_ref):
    out_ref[...] = jnp.zeros_like(out_ref)
    order = sorted(range(panels), key=lambda m: list_rank(panels)[m])
    for m in order:
        at = first_ref[m]
        out_ref[pl.ds(at, slots)] = tiles_ref[m]


def cuts(start, stop, most):
    count = -(-(stop - start) // most)
    ends = [start + (stop - start) * i // count for i in range(count + 1)]
    return [(a, b - a) for a, b in zip(ends[:-1], ends[1:])]


def gather_kernel(n, m, edge, pieces, own_ref, g_ref, hl_ref, hr_ref, zs, zr, xs, xr, local_sem):
    s = lax.axis_index("section")
    c = lax.axis_index("col")
    ring = ({"section": lax.rem(s + 1, n)}, {"section": lax.rem(s + n - 1, n)})
    sides = ({"col": lax.rem(c + 1, m)}, {"col": lax.rem(c + m - 1, m)})
    halo = (hl_ref, hr_ref)
    half = n // 2

    barrier = pltpu.get_barrier_semaphore()
    for who in (*ring, *sides):
        pl.semaphore_signal(barrier, inc=1, device_id=who, device_id_type=MESH)
    pl.semaphore_wait(barrier, 4)

    def shard(way, hop):
        return lax.rem(s + (n - hop if way == 0 else hop), n)

    def source(way, hop, q):
        at, size = pieces[q]
        if hop == 0:
            return own_ref.at[pl.ds(at, size)]
        return g_ref.at[shard(way, hop), pl.ds(at, size)]

    def along(way, hop, q):
        at, size = pieces[q]
        return pltpu.make_async_remote_copy(
            src_ref=source(way, hop, q),
            dst_ref=g_ref.at[shard(way, hop), pl.ds(at, size)],
            send_sem=zs.at[way, hop, q],
            recv_sem=zr.at[way, hop, q],
            device_id=ring[way],
            device_id_type=MESH,
        )

    def across(side, way, hop, q):
        at, size = pieces[q]
        turn = n - 1 if hop == half else hop if way == 0 else half - 1 + hop
        return pltpu.make_async_remote_copy(
            src_ref=source(way, hop, q),
            dst_ref=halo[side].at[shard(way, hop), pl.ds(at, size)],
            send_sem=xs.at[side, turn, q],
            recv_sem=xr.at[side, turn, q],
            device_id=sides[side],
            device_id_type=MESH,
        )

    def travels(way, hop, q):
        return hop < half - 1 or q % 2 == way

    count = len(pieces)
    sent, crossed = [], []
    keep = pltpu.make_async_copy(own_ref.at[pl.ds(0, g_ref.shape[1])], g_ref.at[s], local_sem)
    for hop in range(half + 1):
        for q in range(count):
            for way in (0, 1):
                if hop > 0:
                    if not travels(way, hop - 1, q):
                        continue
                    along(way, hop - 1, q).wait_recv()
                if hop < half and travels(way, hop, q):
                    copy = along(way, hop, q)
                    copy.start()
                    sent.append(copy)
                if pieces[q][0] < edge and (hop > 0 or way == 0):
                    for side in (0, 1):
                        copy = across(side, way, hop, q)
                        copy.start()
                        crossed.append(copy)
        if hop == 0:
            keep.start()
    keep.wait()
    for copy in crossed:
        copy.wait_recv()
    for copy in crossed + sent:
        copy.wait_send()


def expand_kernel(
    n, share, edge, wide, slots, bands, tab_ref, own_ref, g_ref, hl_ref, hr_ref, ranks_ref, out_ref, v_ref, lhs_ref, acc_ref, sems
):
    step = pl.program_id(0)
    s = lax.axis_index("section")
    offs = 2 * W + 1
    across = GROUP + 2 * W
    zero_at = wide + 2 * edge

    @pl.when(step == 0)
    def load():
        copies = [
            pltpu.make_async_copy(g_ref, v_ref.at[:, pl.ds(0, wide)], sems.at[0]),
            pltpu.make_async_copy(hl_ref, v_ref.at[:, pl.ds(wide, edge)], sems.at[1]),
            pltpu.make_async_copy(hr_ref, v_ref.at[:, pl.ds(wide + edge, edge)], sems.at[2]),
        ]
        for copy in copies:
            copy.start()
        v_ref[:, zero_at] = jnp.zeros_like(v_ref[:, zero_at])
        acc_ref[...] = jnp.zeros_like(acc_ref)
        for copy in copies:
            copy.wait()

    tile = n * share
    none = jnp.zeros((tile, tile), v_ref.dtype)
    for a in range(across):
        for p in range(GROUP):
            d = p + W - a
            if abs(d) > W:
                block = jnp.zeros((share, tile), v_ref.dtype)
            else:
                block = v_ref[s, own_ref[(step * GROUP + a) * offs + d + W]]
            lhs_ref[a * share : (a + 1) * share, p * tile : (p + 1) * tile] = block

    def slot(a):
        return lax.rem(step * GROUP + a, across)

    for pair in range(across // 2):
        cols = []
        for b in (2 * pair, 2 * pair + 1):
            rows = []
            for p in range(GROUP):
                e = b - W - p
                if abs(e) > W:
                    rows.append(none)
                else:
                    got = v_ref[:, tab_ref[(step * GROUP + p) * offs + e + W]]
                    rows.append(got.reshape(tile, tile))
            cols.append(jnp.concatenate(rows, axis=0))
        rhs = jnp.concatenate(cols, axis=1)
        res = jnp.dot(lhs_ref[...], rhs, preferred_element_type=jnp.float32)
        for i in (0, 1):
            b = 2 * pair + i
            for a in range(across):
                o = b - a + 2 * W
                if 0 <= o < bands:
                    acc_ref[slot(a), o] += res[a * share : (a + 1) * share, i * tile : (i + 1) * tile]

    @pl.when(step >= 2 * W // GROUP)
    def finish():
        for a in range(GROUP):
            at = slot(a)
            value = acc_ref[at]
            squared = jnp.where(ranks_ref[a] < TOPK, value * value, jnp.float32(0.0))
            totals = jnp.sum(jnp.sum(squared, axis=0), axis=1, keepdims=True)
            out_ref[a] = (squared * (TOPK / (totals + 1e-6))[None]).astype(out_ref.dtype)

    for a in range(GROUP):
        acc_ref[slot(a)] = jnp.zeros(acc_ref.shape[1:], acc_ref.dtype)


def shards(tiles, offsets, counts, ranks):
    panels, slots, share, tile = tiles.shape
    bands = ranks.shape[1]
    total = offsets.shape[0]
    n = lax.axis_size("section")
    m = lax.axis_size("col")
    offs = 2 * W + 1
    edge = 2 * W * slots
    full = panels * slots
    col = lax.axis_index("col")
    first = col * panels

    rank_of = jnp.array(list_rank(panels), jnp.int32)
    before = (rank_of[:, None] < rank_of[None, :]).astype(jnp.float32)
    by_col = counts.reshape(m, panels).astype(jnp.float32)
    starts = jnp.dot(by_col, before, preferred_element_type=jnp.float32).astype(jnp.int32)
    most = jnp.max(jnp.sum(counts.reshape(m, panels), axis=1))

    packed = pl.pallas_call(
        functools.partial(pack_kernel, panels, slots),
        out_shape=jax.ShapeDtypeStruct((full + slots, share, tile), tiles.dtype),
        in_specs=[pl.BlockSpec(memory_space=pltpu.SMEM), pl.BlockSpec(memory_space=pltpu.VMEM)],
        out_specs=pl.BlockSpec(memory_space=pltpu.VMEM),
        name="pack",
    )(lax.dynamic_index_in_dim(starts, col, 0, False), tiles)

    reach = panels + 2 * W
    where = first - 3 * W + W + jnp.arange(reach, dtype=jnp.int32) + W
    at = jnp.clip(where, 0, total - 1)
    win_off = offsets[at]
    win_cnt = jnp.where((where >= 0) & (where < total), counts[at], 0)
    win_start = starts.reshape(total)[at]
    ids = jnp.arange(slots, dtype=jnp.int32)
    rows = where[:, None] + win_off
    ok = (ids[None] < win_cnt[:, None]) & (rows >= 0) & (rows < total)
    hit = ok[:, None, :] & (win_off[:, None, :] == jnp.arange(-W, W + 1, dtype=jnp.int32)[None, :, None])
    found = jnp.sum(jnp.where(hit, ids[None, None] + 1, 0), axis=2)

    def level(wide):
        pieces = cuts(0, edge, 48) + cuts(edge, wide, 64)
        count = len(pieces)
        edges = sum(1 for at, _ in pieces if at < edge)

        def run(packed, found, win_start, ranks):
            base = jnp.where(where < first, wide, jnp.where(where < first + panels, 0, wide + edge))
            none = wide + 2 * edge
            tab = jnp.where(found > 0, (base + win_start)[:, None] + found - 1, none)
            mine = jnp.full((panels + 4 * W, offs), none, jnp.int32)
            mine = lax.dynamic_update_slice(mine, tab[W : W + panels], (2 * W, 0))
            g, hl, hr = pl.pallas_call(
                functools.partial(gather_kernel, n, m, edge, pieces),
                out_shape=(
                    jax.ShapeDtypeStruct((n, wide, share, tile), tiles.dtype),
                    jax.ShapeDtypeStruct((n, edge, share, tile), tiles.dtype),
                    jax.ShapeDtypeStruct((n, edge, share, tile), tiles.dtype),
                ),
                in_specs=[pl.BlockSpec(memory_space=pltpu.VMEM)],
                out_specs=(pl.BlockSpec(memory_space=pl.ANY),) * 3,
                scratch_shapes=[
                    pltpu.SemaphoreType.DMA((2, n // 2, count)),
                    pltpu.SemaphoreType.DMA((2, n // 2, count)),
                    pltpu.SemaphoreType.DMA((2, n, edges)),
                    pltpu.SemaphoreType.DMA((2, n, edges)),
                    pltpu.SemaphoreType.DMA,
                ],
                compiler_params=pltpu.CompilerParams(collective_id=wide // 16, has_side_effects=True),
                name=f"gather{wide}",
            )(packed)
            steps = reach // GROUP
            lag = 2 * W // GROUP
            block = pl.BlockSpec((GROUP, bands, share, tile), lambda i, *_: (jnp.maximum(i - lag, 0), 0, 0, 0))
            return pl.pallas_call(
                functools.partial(expand_kernel, n, share, edge, wide, slots, bands),
                out_shape=jax.ShapeDtypeStruct(ranks.shape, jnp.bfloat16),
                grid_spec=pltpu.PrefetchScalarGridSpec(
                    num_scalar_prefetch=2,
                    grid=(steps,),
                    in_specs=[pl.BlockSpec(memory_space=pl.ANY)] * 3 + [block],
                    out_specs=block,
                    scratch_shapes=[
                        pltpu.VMEM((n, wide + 2 * edge + 1, share, tile), tiles.dtype),
                        pltpu.VMEM(((GROUP + 2 * W) * share, GROUP * tile), tiles.dtype),
                        pltpu.VMEM((GROUP + 2 * W, bands, share, tile), jnp.float32),
                        pltpu.SemaphoreType.DMA((3,)),
                    ],
                ),
                compiler_params=pltpu.CompilerParams(vmem_limit_bytes=60 * 1024 * 1024),
                name=f"expand{wide}",
            )(tab.reshape(-1), mine.reshape(-1), g, hl, hr, ranks)

        return run

    wides = [full * i // 12 for i in (6, 7, 8, 9, 12)]
    pick = sum((most > wide).astype(jnp.int32) for wide in wides[:-1])
    return lax.switch(pick, [level(wide) for wide in wides], packed, found, win_start, ranks)


def solution(mesh):
    placed = (P("col", None, "section", None), P(), P(), P("col", None, "section", None))
    return jax.shard_map(
        shards,
        mesh=mesh,
        in_specs=placed,
        out_specs=P("col", None, "section", None),
        check_vma=False,
    )
```

```python
import functools

import jax
import jax.numpy as jnp
from jax import lax
from jax.experimental import pallas as pl
from jax.experimental.pallas import tpu as pltpu
from jax.sharding import PartitionSpec as P

W = 6
TOPK = 256
GROUP = 8
STRIDE = 16
WIDES = (192, 224, 240, 256, 272, 288, 320)
MESH = pl.DeviceIdType.MESH


def plan_kernel(m, wides, edge, counts_ref, offsets_ref, lanes_ref, tiles_ref, packed_ref, tab_ref, pick_ref):
    panels, slots = tiles_ref.shape[:2]
    col = lax.axis_index("col")
    none = 2 * edge
    base = none + 1

    def run(row, count, owner, begin, at, region, pack):
        valid = (owner >= 0) & (owner < m)
        lead = jnp.clip(owner, 0, m - 1) * panels + begin

        def panel(i, at):
            p = lead + i
            used = jnp.where(valid, counts_ref[p], 0)
            line = (row + i) * STRIDE + W
            place = region + at
            left = line
            for k in range(slots):
                off = offsets_ref[k, p]
                tab_ref[line + off] = jnp.where(k < used, place + k, none)
                left = left - off
            tab_ref[left] = none
            if pack:
                packed_ref[pl.ds(at, slots)] = tiles_ref[begin + i]
            return at + used

        return lax.fori_loop(0, count, panel, at)

    at = run(W, W, col, 0, 0, base, True)
    at = run(panels, W, col, panels - W, at, base, True)
    run(2 * W, panels - 2 * W, col, W, at, base, True)
    lead = jnp.maximum(col - 1, 0) * panels
    ahead = counts_ref[lead]
    for i in range(1, W):
        ahead = ahead + counts_ref[lead + i]
    run(0, W, col - 1, panels - W, ahead, 0, False)
    run(W + panels, W, col + 1, 0, 0, edge, False)

    @pl.when(col == 0)
    def top():
        for i in range(W):
            for e in range(W - i):
                tab_ref[(W + i) * STRIDE + e] = none

    @pl.when(col == m - 1)
    def bottom():
        for i in range(W):
            for e in range(W - i):
                tab_ref[(W + panels - 1 - i) * STRIDE + 2 * W - e] = none

    same = lax.broadcasted_iota(jnp.int32, (128, 128), 0) // panels == lax.broadcasted_iota(jnp.int32, (128, 128), 1) // panels
    sums = jnp.dot(
        lanes_ref[...].astype(jnp.float32).astype(jnp.bfloat16),
        same.astype(jnp.float32).astype(jnp.bfloat16),
        preferred_element_type=jnp.float32,
    )
    most = jnp.max(sums).astype(jnp.int32)
    pick = 0
    for wide in wides[:-1]:
        pick = pick + (most > wide).astype(jnp.int32)
    pick_ref[0] = pick


def cuts(start, stop, most):
    count = -(-(stop - start) // most)
    ends = [start + (stop - start) * i // count for i in range(count + 1)]
    return [(a, b - a) for a, b in zip(ends[:-1], ends[1:])]


def gather_kernel(n, m, edge, wide, pieces, own_ref, v_ref, zs, zr, xs, xr):
    s = lax.axis_index("section")
    c = lax.axis_index("col")
    ring = ({"section": lax.rem(s + 1, n)}, {"section": lax.rem(s + n - 1, n)})
    sides = ({"col": lax.rem(c + 1, m)}, {"col": lax.rem(c + m - 1, m)})
    zero_at = 2 * edge
    base = zero_at + 1
    half = n // 2

    barrier = pltpu.get_barrier_semaphore()
    for who in (*ring, *sides):
        pl.semaphore_signal(barrier, inc=1, device_id=who, device_id_type=MESH)
    pl.semaphore_wait(barrier, 4)

    def shard(way, hop):
        return lax.rem(s + (n - hop if way == 0 else hop), n)

    def source(way, hop, q):
        at, size = pieces[q]
        if hop == 0:
            return own_ref.at[pl.ds(at, size)]
        return v_ref.at[shard(way, hop), pl.ds(base + at, size)]

    def along(way, hop, q):
        at, size = pieces[q]
        return pltpu.make_async_remote_copy(
            src_ref=source(way, hop, q),
            dst_ref=v_ref.at[shard(way, hop), pl.ds(base + at, size)],
            send_sem=zs.at[way, hop, q],
            recv_sem=zr.at[way, hop, q],
            device_id=ring[way],
            device_id_type=MESH,
        )

    def across(side, way, hop, q):
        at, size = pieces[q]
        turn = n - 1 if hop == half else hop if way == 0 else half - 1 + hop
        return pltpu.make_async_remote_copy(
            src_ref=source(way, hop, q),
            dst_ref=v_ref.at[shard(way, hop), pl.ds(side * edge + at, size)],
            send_sem=xs.at[side, turn, q],
            recv_sem=xr.at[side, turn, q],
            device_id=sides[side],
            device_id_type=MESH,
        )

    def travels(way, hop, q):
        return hop < half - 1 or q % 2 == way

    count = len(pieces)
    sent, crossed = [], []
    for hop in range(half + 1):
        for q in range(count):
            for way in (0, 1):
                if hop > 0:
                    if not travels(way, hop - 1, q):
                        continue
                    along(way, hop - 1, q).wait_recv()
                if hop < half and travels(way, hop, q):
                    copy = along(way, hop, q)
                    copy.start()
                    sent.append(copy)
                if pieces[q][0] < edge and (hop > 0 or way == 0):
                    for side in (0, 1):
                        copy = across(side, way, hop, q)
                        copy.start()
                        crossed.append(copy)
        if hop == 0:
            v_ref[:, zero_at] = jnp.zeros_like(v_ref[:, zero_at])
            v_ref[s, pl.ds(base, wide)] = own_ref[pl.ds(0, wide)]
    for copy in crossed:
        copy.wait_recv()
    for copy in crossed + sent:
        copy.wait_send()


def expand_kernel(n, bands, tab_ref, v_ref, ranks_ref, out_ref, lhs_ref, sq_ref):
    step = pl.program_id(0)
    s = lax.axis_index("section")
    share, tile = v_ref.shape[2:]
    mids = GROUP + 2 * W
    ends = GROUP + 4 * W

    def where(p, e):
        return tab_ref[(step * GROUP + p) * STRIDE + e + W]

    for a in range(GROUP):
        for p in range(mids):
            d = p - W - a
            rows, cols = slice(a * share, (a + 1) * share), slice(p * tile, (p + 1) * tile)
            if abs(d) <= W:
                lhs_ref[rows, cols] = v_ref[s, where(a + W, d)]
            else:
                lhs_ref[rows, cols] = jnp.zeros((share, tile), lhs_ref.dtype)

    empty = jnp.zeros((tile, tile), v_ref.dtype)
    sums = [jnp.zeros((share, tile), jnp.float32) for _ in range(GROUP)]
    for b in range(0, ends, 2):
        lo, hi = max(0, b - 2 * W), min(mids, b + 2)
        sides = []
        for r in (b, b + 1):
            rows = []
            for p in range(lo, hi):
                e = r - W - p
                if abs(e) <= W:
                    rows.append(v_ref[:, where(p, e)].reshape(tile, tile))
                else:
                    rows.append(empty)
            sides.append(jnp.concatenate(rows, axis=0))
        res = jnp.dot(
            lhs_ref[:, lo * tile : hi * tile],
            jnp.concatenate(sides, axis=1),
            preferred_element_type=jnp.float32,
        )
        for i in (0, 1):
            for a in range(GROUP):
                o = b + i - a
                if 0 <= o < bands:
                    value = res[a * share : (a + 1) * share, i * tile : (i + 1) * tile]
                    squared = jnp.where(ranks_ref[step * GROUP + a, o] < TOPK, value * value, jnp.float32(0.0))
                    sq_ref[a, o] = squared
                    sums[a] = sums[a] + squared
    for a in range(GROUP):
        totals = jnp.sum(sums[a], axis=1, keepdims=True)
        out_ref[a] = (sq_ref[a] * (TOPK / (totals + 1e-6))[None]).astype(out_ref.dtype)


def shards(tiles, offsets, counts, ranks):
    panels, slots, share, tile = tiles.shape
    bands = ranks.shape[1]
    n = lax.axis_size("section")
    m = lax.axis_size("col")
    edge = 2 * W * slots
    full = panels * slots
    wides = [w for w in WIDES if edge < w < full] + [full]
    scalars = pl.BlockSpec(memory_space=pltpu.SMEM)
    near = pl.BlockSpec(memory_space=pltpu.VMEM)

    packed, tab, pick = pl.pallas_call(
        functools.partial(plan_kernel, m, wides, edge),
        out_shape=(
            jax.ShapeDtypeStruct((full + slots, share, tile), tiles.dtype),
            jax.ShapeDtypeStruct(((panels + 2 * W) * STRIDE,), jnp.int32),
            jax.ShapeDtypeStruct((1,), jnp.int32),
        ),
        in_specs=[scalars, scalars, near, near],
        out_specs=(near, scalars, scalars),
        compiler_params=pltpu.CompilerParams(vmem_limit_bytes=8 << 20),
        name="plan",
    )(counts, offsets.T, counts.reshape(-1, 128), tiles)

    def level(wide):
        pieces = cuts(0, edge, 48) + cuts(edge, wide, 64)
        count = len(pieces)
        edges = sum(1 for at, _ in pieces if at < edge)

        def run(packed, tab, ranks):
            v = pl.pallas_call(
                functools.partial(gather_kernel, n, m, edge, wide, pieces),
                out_shape=jax.ShapeDtypeStruct((n, 2 * edge + 1 + wide, share, tile), tiles.dtype),
                in_specs=[near],
                out_specs=near,
                scratch_shapes=[
                    pltpu.SemaphoreType.DMA((2, n // 2, count)),
                    pltpu.SemaphoreType.DMA((2, n // 2, count)),
                    pltpu.SemaphoreType.DMA((2, n, edges)),
                    pltpu.SemaphoreType.DMA((2, n, edges)),
                ],
                compiler_params=pltpu.CompilerParams(
                    collective_id=wide // 8, has_side_effects=True, vmem_limit_bytes=8 << 20
                ),
                name=f"gather{wide}",
            )(packed)
            block = pl.BlockSpec((GROUP, bands, share, tile), lambda i, *_: (i, 0, 0, 0))
            return pl.pallas_call(
                functools.partial(expand_kernel, n, bands),
                out_shape=pltpu.HBM(ranks.shape, jnp.bfloat16),
                grid_spec=pltpu.PrefetchScalarGridSpec(
                    num_scalar_prefetch=1,
                    grid=(panels // GROUP,),
                    in_specs=[near, near],
                    out_specs=block,
                    scratch_shapes=[
                        pltpu.VMEM((GROUP * share, (GROUP + 2 * W) * tile), tiles.dtype),
                        pltpu.VMEM((GROUP, bands, share, tile), jnp.float32),
                    ],
                ),
                compiler_params=pltpu.CompilerParams(vmem_limit_bytes=30 << 20),
                name=f"expand{wide}",
            )(tab, v, ranks)

        return run

    return lax.switch(pick[0], [level(wide) for wide in wides], packed, tab, ranks)


def solution(mesh):
    placed = (P("col", None, "section", None), P(), P(), P("col", None, "section", None))
    return jax.shard_map(
        shards,
        mesh=mesh,
        in_specs=placed,
        out_specs=P("col", None, "section", None),
        check_vma=False,
    )
```

```python
import functools

import jax
import jax.numpy as jnp
from jax import lax
from jax.experimental import pallas as pl
from jax.experimental.pallas import tpu as pltpu
from jax.sharding import PartitionSpec as P

W = 6
TOPK = 256
GROUP = 8
STRIDE = 16
WIDES = (208, 216, 224, 232, 240, 248, 256, 280, 320)
MESH = pl.DeviceIdType.MESH


def plan_kernel(
    m, wides, brink, counts_in, offsets_in, lanes_in, tiles_in, packed_ref, tab_ref, pick_ref, counts_ref, offsets_ref, lanes_ref, tiles_ref, sems
):
    copies = [
        pltpu.make_async_copy(src, dst, sems.at[i])
        for i, (src, dst) in enumerate(
            ((counts_in, counts_ref), (offsets_in, offsets_ref), (lanes_in, lanes_ref), (tiles_in, tiles_ref))
        )
    ]
    for copy in copies:
        copy.start()
    panels, slots = tiles_ref.shape[:2]
    col = lax.axis_index("col")
    me = lax.rem(col, 2)
    rest = panels - W
    none = brink

    copies[2].wait()
    pair = lax.broadcasted_iota(jnp.int32, (128, 128), 0) // (2 * panels)
    same = pair == lax.broadcasted_iota(jnp.int32, (128, 128), 1) // (2 * panels)
    sums = jnp.dot(
        lanes_ref[...].astype(jnp.float32).astype(jnp.bfloat16),
        same.astype(jnp.float32).astype(jnp.bfloat16),
        preferred_element_type=jnp.float32,
    )
    most = jnp.max(sums).astype(jnp.int32)
    pick, wide = 0, wides[0]
    for now, then in zip(wides[:-1], wides[1:]):
        over = most > 2 * now
        pick = pick + over.astype(jnp.int32)
        wide = jnp.where(over, then, wide)

    copies[0].wait()
    copies[1].wait()
    other = (col + 1 - 2 * me) * panels
    front = counts_ref[other]
    for i in range(1, rest):
        front = front + counts_ref[other + i]
    back = counts_ref[other + rest]
    for i in range(rest + 1, panels):
        back = back + counts_ref[other + i]
    pick_ref[0] = pick
    pick_ref[1] = front + back - wide

    mine = brink + 1 + me * wide
    theirs = brink + 1 + (1 - me) * wide

    def run(row, count, lead, at, straight, folded, valid=None, pack=None):
        turned = folded + 2 * wide - 1

        def panel(i, at):
            p = lead + i
            used = counts_ref[p]
            if valid is not None:
                used = jnp.where(valid, used, 0)
            line = (row + i) * STRIDE + W
            left = line
            for k in range(slots):
                off = offsets_ref[k, p]
                x = at + k
                place = straight + x if valid is not None else jnp.where(x < wide, straight + x, turned - x)
                tab_ref[line + off] = jnp.where(k < used, place, none)
                left = left - off
            tab_ref[left] = none
            if pack is not None:
                packed_ref[pl.ds(at, slots)] = tiles_ref[pack + i]
            return at + used

        return lax.fori_loop(0, count, panel, at)

    run(jnp.where(me == 0, W + panels, 0), W, other + me * rest, jnp.where(me == 0, back, front), theirs, mine)
    outer = col - 1 + 2 * me
    run(
        jnp.where(me == 0, 0, W + panels),
        W,
        jnp.clip(outer, 0, m - 1) * panels + (1 - me) * rest,
        0,
        0,
        0,
        valid=(outer >= 0) & (outer < m),
    )
    copies[3].wait()
    at = run(W + me * rest, W, col * panels + me * rest, 0, mine, theirs, pack=me * rest)
    begin = (1 - me) * W
    run(W + begin, rest, col * panels + begin, at, mine, theirs, pack=begin)

    @pl.when(col == 0)
    def top():
        for i in range(W):
            for e in range(W - i):
                tab_ref[(W + i) * STRIDE + e] = none

    @pl.when(col == m - 1)
    def bottom():
        for i in range(W):
            for e in range(W - i):
                tab_ref[(W + panels - 1 - i) * STRIDE + 2 * W - e] = none


def cuts(marks, most):
    out = []
    for start, stop in zip(marks[:-1], marks[1:]):
        count = -(-(stop - start) // most)
        ends = [start + (stop - start) * i // count for i in range(count + 1)]
        out += [(a, b - a) for a, b in zip(ends[:-1], ends[1:])]
    return out


def gather_kernel(
    n, m, brink, wide, full, pieces, packed_ref, pick_ref, v_ref, extra_ref, zs, zr, ts, tr, xs, xr, es, er
):
    s = lax.axis_index("section")
    c = lax.axis_index("col")
    me = lax.rem(c, 2)
    ring = ({"section": lax.rem(s + 1, n)}, {"section": lax.rem(s + n - 1, n)})
    twin = {"col": c + 1 - 2 * me}
    outer = {"col": lax.rem(c + m - 1 + 2 * me, m)}
    base = brink + 1 + me * wide
    half = n // 2
    pure = 2 * wide - full
    spare = full - wide

    barrier = pltpu.get_barrier_semaphore()
    for who in (*ring, twin, outer):
        pl.semaphore_signal(barrier, inc=1, device_id=who, device_id_type=MESH)
    pl.semaphore_wait(barrier, 4)

    def shard(way, hop):
        return lax.rem(s + (n - hop if way == 0 else hop), n)

    def send(way, hop, q, at_there, send_sem, recv_sem, who):
        at, size = pieces[q]
        if hop == 0 and at + size <= pure:
            src = packed_ref.at[pl.ds(at, size)]
        else:
            src = v_ref.at[shard(way, hop), pl.ds(base + at, size)]
        return pltpu.make_async_remote_copy(
            src_ref=src,
            dst_ref=v_ref.at[shard(way, hop), pl.ds(at_there + at, size)],
            send_sem=send_sem,
            recv_sem=recv_sem,
            device_id=who,
            device_id_type=MESH,
        )

    def along(way, hop, q):
        return send(way, hop, q, base, zs.at[way, hop, q], zr.at[way, hop, q], ring[way])

    def turn(way, hop):
        return n - 1 if hop == half else hop if way == 0 else half - 1 + hop

    def share(way, hop, q):
        return send(way, hop, q, base, ts.at[turn(way, hop), q], tr.at[turn(way, hop), q], twin)

    def across(way, hop, q):
        return send(way, hop, q, 0, xs.at[turn(way, hop), q], xr.at[turn(way, hop), q], outer)

    def travels(way, hop, q):
        return hop < half - 1 or q % 2 == way

    sent, crossed = [], []

    def pass_on(hop, q):
        for way in (0, 1):
            if hop > 0:
                if not travels(way, hop - 1, q):
                    continue
                along(way, hop - 1, q).wait_recv()
            if hop < half and travels(way, hop, q):
                sent.append(along(way, hop, q))
                sent[-1].start()
            if hop > 0 or way == 0:
                if pieces[q][0] < brink:
                    crossed.append(across(way, hop, q))
                    crossed[-1].start()
                crossed.append(share(way, hop, q))
                crossed[-1].start()

    early = [q for q, (at, size) in enumerate(pieces) if at + size <= pure]
    late = [q for q in range(len(pieces)) if q not in early]
    if spare:
        swap = pltpu.make_async_remote_copy(
            src_ref=packed_ref.at[pl.ds(wide, spare)],
            dst_ref=extra_ref,
            send_sem=es,
            recv_sem=er,
            device_id=twin,
            device_id_type=MESH,
        )
        swap.start()
    for q in early:
        pass_on(0, q)
    if spare:
        swap.wait_recv()

        def merge(i, carry):
            kept = packed_ref[wide - 1 - i]
            v_ref[s, base + wide - 1 - i] = jnp.where(i < pick_ref[1], extra_ref[i], kept)
            return carry

        lax.fori_loop(0, spare, merge, 0, unroll=8)
    for q in late:
        pass_on(0, q)
    v_ref[s, pl.ds(base, pure)] = packed_ref[pl.ds(0, pure)]
    v_ref[:, brink] = jnp.zeros_like(v_ref[:, brink])
    for hop in range(1, half + 1):
        for q in range(len(pieces)):
            pass_on(hop, q)
    for copy in crossed:
        copy.wait_recv()
    for copy in crossed + sent:
        copy.wait_send()
    if spare:
        swap.wait_send()


def expand_kernel(n, bands, tab_ref, v_ref, ranks_ref, out_ref, lhs_ref, sq_ref):
    step = pl.program_id(0)
    s = lax.axis_index("section")
    share, tile = v_ref.shape[2:]
    mids = GROUP + 2 * W
    ends = GROUP + 4 * W

    def where(p, e):
        return tab_ref[(step * GROUP + p) * STRIDE + e + W]

    for a in range(GROUP):
        for p in range(mids):
            d = p - W - a
            rows, cols = slice(a * share, (a + 1) * share), slice(p * tile, (p + 1) * tile)
            if abs(d) <= W:
                lhs_ref[rows, cols] = v_ref[s, where(a + W, d)]
            else:
                lhs_ref[rows, cols] = jnp.zeros((share, tile), lhs_ref.dtype)

    empty = jnp.zeros((tile, tile), v_ref.dtype)
    sums = [jnp.zeros((share, tile), jnp.float32) for _ in range(GROUP)]
    for b in range(0, ends, 2):
        lo, hi = max(0, b - 2 * W), min(mids, b + 2)
        sides = []
        for r in (b, b + 1):
            rows = []
            for p in range(lo, hi):
                e = r - W - p
                if abs(e) <= W:
                    rows.append(v_ref[:, where(p, e)].reshape(tile, tile))
                else:
                    rows.append(empty)
            sides.append(jnp.concatenate(rows, axis=0))
        res = jnp.dot(
            lhs_ref[:, lo * tile : hi * tile],
            jnp.concatenate(sides, axis=1),
            preferred_element_type=jnp.float32,
        )
        for i in (0, 1):
            for a in range(GROUP):
                o = b + i - a
                if 0 <= o < bands:
                    value = res[a * share : (a + 1) * share, i * tile : (i + 1) * tile]
                    squared = jnp.where(ranks_ref[step * GROUP + a, o] < TOPK, value * value, jnp.float32(0.0))
                    sq_ref[a, o] = squared
                    sums[a] = sums[a] + squared
    for a in range(GROUP):
        totals = jnp.sum(sums[a], axis=1, keepdims=True)
        out_ref[a] = (sq_ref[a] * (TOPK / (totals + 1e-6))[None]).astype(out_ref.dtype)


def shards(tiles, offsets, counts, ranks):
    panels, slots, share, tile = tiles.shape
    bands = ranks.shape[1]
    n = lax.axis_size("section")
    m = lax.axis_size("col")
    brink = W * slots
    full = panels * slots
    wides = [w for w in WIDES if full // 2 < w < full] + [full]
    scalars = pl.BlockSpec(memory_space=pltpu.SMEM)
    near = pl.BlockSpec(memory_space=pltpu.VMEM)
    far = pl.BlockSpec(memory_space=pltpu.HBM)

    packed, tab, pick = pl.pallas_call(
        functools.partial(plan_kernel, m, wides, brink),
        out_shape=(
            jax.ShapeDtypeStruct((full + slots, share, tile), tiles.dtype),
            jax.ShapeDtypeStruct(((panels + 2 * W) * STRIDE,), jnp.int32),
            jax.ShapeDtypeStruct((2,), jnp.int32),
        ),
        in_specs=[far] * 4,
        out_specs=(near, scalars, scalars),
        scratch_shapes=[
            pltpu.SMEM(counts.shape, jnp.int32),
            pltpu.SMEM(offsets.shape[::-1], jnp.int32),
            pltpu.VMEM((counts.size // 128, 128), jnp.int32),
            pltpu.VMEM(tiles.shape, tiles.dtype),
            pltpu.SemaphoreType.DMA((4,)),
        ],
        compiler_params=pltpu.CompilerParams(vmem_limit_bytes=8 << 20),
        name="plan",
    )(*(pltpu.with_memory_space_constraint(x, pltpu.HBM) for x in (counts, offsets.T, counts.reshape(-1, 128), tiles)))

    def level(wide):
        pure = 2 * wide - full
        pieces = cuts(sorted({0, pure, min(brink, wide), wide}), 48)
        count = len(pieces)
        edges = sum(1 for at, _ in pieces if at < brink)

        def run(packed, tab, pick, ranks):
            v = pl.pallas_call(
                functools.partial(gather_kernel, n, m, brink, wide, full, pieces),
                out_shape=jax.ShapeDtypeStruct((n, brink + 1 + 2 * wide, share, tile), tiles.dtype),
                in_specs=[near, scalars],
                out_specs=near,
                scratch_shapes=[pltpu.VMEM((max(full - wide, 1), share, tile), tiles.dtype)]
                + [pltpu.SemaphoreType.DMA((2, n // 2, count))] * 2
                + [pltpu.SemaphoreType.DMA((n, count))] * 2
                + [pltpu.SemaphoreType.DMA((n, edges))] * 2
                + [pltpu.SemaphoreType.DMA] * 2,
                compiler_params=pltpu.CompilerParams(
                    collective_id=wides.index(wide), has_side_effects=True, vmem_limit_bytes=4 << 20
                ),
                name=f"gather{wide}",
            )(packed, pick)
            block = pl.BlockSpec((GROUP, bands, share, tile), lambda i, *_: (i, 0, 0, 0))
            return pl.pallas_call(
                functools.partial(expand_kernel, n, bands),
                out_shape=pltpu.HBM(ranks.shape, jnp.bfloat16),
                grid_spec=pltpu.PrefetchScalarGridSpec(
                    num_scalar_prefetch=1,
                    grid=(panels // GROUP,),
                    in_specs=[near, near],
                    out_specs=block,
                    scratch_shapes=[
                        pltpu.VMEM((GROUP * share, (GROUP + 2 * W) * tile), tiles.dtype),
                        pltpu.VMEM((GROUP, bands, share, tile), jnp.float32),
                    ],
                ),
                compiler_params=pltpu.CompilerParams(vmem_limit_bytes=20 << 20),
                name=f"expand{wide}",
            )(tab, v, ranks)

        return run

    return lax.switch(pick[0], [level(wide) for wide in wides], packed, tab, pick, ranks)


def solution(mesh):
    placed = (P("col", None, "section", None), P(), P(), P("col", None, "section", None))
    return jax.shard_map(
        shards,
        mesh=mesh,
        in_specs=placed,
        out_specs=P("col", None, "section", None),
        check_vma=False,
    )
```

```python
import functools

import jax
import jax.numpy as jnp
from jax import lax
from jax.experimental import pallas as pl
from jax.experimental.pallas import tpu as pltpu
from jax.sharding import PartitionSpec as P

W = 6
TOPK = 256
GROUP = 8
STRIDE = 16
WIDES = (208, 216, 224, 232, 240, 252, 288)
MESH = pl.DeviceIdType.MESH


def plan_kernel(m, wides, counts_in, lanes_in, tiles_in, packed_ref, pick_ref, counts_ref, lanes_ref, tiles_ref, sems):
    copies = [
        pltpu.make_async_copy(src, dst, sems.at[i])
        for i, (src, dst) in enumerate(((tiles_in, tiles_ref), (counts_in, counts_ref), (lanes_in, lanes_ref)))
    ]
    for copy in copies:
        copy.start()
    panels, slots = tiles_ref.shape[:2]
    col = lax.axis_index("col")
    me = lax.rem(col, 2)

    pair = lax.broadcasted_iota(jnp.int32, (128, 128), 0) // (2 * panels)
    same = pair == lax.broadcasted_iota(jnp.int32, (128, 128), 1) // (2 * panels)
    same = same.astype(jnp.float32).astype(jnp.bfloat16)
    copies[1].wait()
    copies[2].wait()
    sums = jnp.dot(
        lanes_ref[...].astype(jnp.float32).astype(jnp.bfloat16), same, preferred_element_type=jnp.float32
    )
    most = jnp.max(sums).astype(jnp.int32)
    other = (col + 1 - 2 * me) * panels
    theirs = counts_ref[other]
    for i in range(1, panels):
        theirs = theirs + counts_ref[other + i]

    copies[0].wait()

    def run(count, begin, at):
        def panel(i, at):
            packed_ref[pl.ds(at, slots)] = tiles_ref[begin + i]
            return at + counts_ref[col * panels + begin + i]

        return lax.fori_loop(0, count, panel, at, unroll=2)

    at = run(W, me * (panels - W), 0)
    run(panels - W, (1 - me) * W, at)

    pick, wide = 0, wides[0]
    for now, then in zip(wides[:-1], wides[1:]):
        over = most > 2 * now
        pick = pick + over.astype(jnp.int32)
        wide = jnp.where(over, then, wide)
    pick_ref[0] = pick
    pick_ref[1] = theirs - wide


def cuts(marks, most):
    out = []
    for start, stop in zip(marks[:-1], marks[1:]):
        count = -(-(stop - start) // most)
        ends = [start + (stop - start) * i // count for i in range(count + 1)]
        out += [(a, b - a) for a, b in zip(ends[:-1], ends[1:])]
    return out


def table(m, brink, wide, full, sources, places, sems, tab_ref):
    copies = [pltpu.make_async_copy(src, dst, sems.at[i]) for i, (src, dst) in enumerate(zip(sources, places))]
    for copy in copies:
        copy.start()
    for copy in copies:
        copy.wait()
    counts_ref, offsets_ref = places
    slots, total = offsets_ref.shape
    panels = total // m
    rest = panels - W
    col = lax.axis_index("col")
    first = col * panels
    reach = min(256, total)
    lanes = tab_ref.shape[1]
    start = jnp.clip((first - panels + total) // 128 * 128 - total, 0, total - reach)
    start = pl.multiple_of(start, 128)
    exact = lambda x: x.astype(jnp.float32).astype(jnp.bfloat16)
    counts = exact(jnp.broadcast_to(counts_ref[:, pl.ds(start, reach)], (8, reach)))
    offsets = exact(offsets_ref[:, pl.ds(start, reach)])

    def order(p):
        owner = (p + total) // panels
        at = p + total - owner * panels
        core = lax.rem(owner, 2)
        return owner, core, jnp.where(core == 0, at, jnp.where(at >= rest, at - rest, at + W))

    shape = (reach, lanes)
    here = start + lax.broadcasted_iota(jnp.int32, shape, 0)
    there = first - W + lax.broadcasted_iota(jnp.int32, shape, 1) // STRIDE
    own_h, _, rank_h = order(here)
    own_t, _, rank_t = order(there)
    pickers = exact((here == there).astype(jnp.int32))
    earlier = exact(((own_h == own_t) & (rank_h < rank_t)).astype(jnp.int32))

    def times(a, b):
        return jnp.dot(a, b, preferred_element_type=jnp.float32)

    offs = times(offsets, pickers)
    used = times(counts, pickers)[:1]
    ahead = times(counts, earlier)[:1]
    lane = lax.broadcasted_iota(jnp.int32, (1, lanes), 1)
    there = first - W + lane // STRIDE
    e = lax.rem(lane, STRIDE) - W
    owner, core, _ = order(there)
    k = lax.broadcasted_iota(jnp.int32, (slots, lanes), 0).astype(jnp.float32)
    hit = (offs == e.astype(jnp.float32)) & (k < used)
    found = jnp.sum(jnp.where(hit, k + 1.0, 0.0), axis=0, keepdims=True)
    x = (ahead + found - 1.0).astype(jnp.int32)
    straight = brink + 1 + core * wide + x
    folded = brink + 1 + (1 - core) * wide + 2 * wide - 1 - x
    place = jnp.where(x < wide, straight, folded)
    inner = (owner // 2) == (col + m) // 2
    place = jnp.where(inner, place, x)
    row = there + e
    ok = (found > 0.0) & (there >= 0) & (there < total) & (row >= 0) & (row < total)
    tab_ref[...] = jnp.where(ok, place, brink)


def gather_kernel(
    n, m, brink, wide, full, pieces, packed_ref, pick_ref, counts_in, offsets_in, ranks_in, v_ref, tab_ref, ranks_ref, extra_ref, counts_ref, offsets_ref, ls, zs, zr, ts, tr, xs, xr, es, er
):
    s = lax.axis_index("section")
    c = lax.axis_index("col")
    me = lax.rem(c, 2)
    ring = ({"section": lax.rem(s + 1, n)}, {"section": lax.rem(s + n - 1, n)})
    twin = {"col": c + 1 - 2 * me}
    outer = {"col": lax.rem(c + m - 1 + 2 * me, m)}
    base = brink + 1 + me * wide
    half = n // 2
    pure = 2 * wide - full
    spare = full - wide

    fetch = pltpu.make_async_copy(ranks_in, ranks_ref, ls.at[2])
    fetch.start()
    barrier = pltpu.get_barrier_semaphore()
    for who in (*ring, twin, outer):
        pl.semaphore_signal(barrier, inc=1, device_id=who, device_id_type=MESH)
    pl.semaphore_wait(barrier, 4)

    def shard(way, hop):
        return lax.rem(s + (n - hop if way == 0 else hop), n)

    def span(way, hop, q):
        at, size = pieces[q]
        if hop < half:
            return at, size
        return (at, size - size // 2) if way == 0 else (at + size - size // 2, size // 2)

    def send(way, hop, span, at_there, send_sem, recv_sem, who):
        at, size = span
        if hop == 0 and at + size <= pure:
            src = packed_ref.at[pl.ds(at, size)]
        else:
            src = v_ref.at[shard(way, hop), pl.ds(base + at, size)]
        return pltpu.make_async_remote_copy(
            src_ref=src,
            dst_ref=v_ref.at[shard(way, hop), pl.ds(at_there + at, size)],
            send_sem=send_sem,
            recv_sem=recv_sem,
            device_id=who,
            device_id_type=MESH,
        )

    def along(way, hop, q):
        return send(way, hop, span(way, hop + 1, q), base, zs.at[way, hop, q], zr.at[way, hop, q], ring[way])

    def turn(way, hop):
        return hop if way == 0 else half + hop

    def share(way, hop, q):
        at = turn(way, hop)
        return send(way, hop, span(way, hop, q), base, ts.at[at, q], tr.at[at, q], twin)

    def across(way, hop, q):
        at = turn(way, hop)
        return send(way, hop, span(way, hop, q), 0, xs.at[at, q], xr.at[at, q], outer)

    sent, crossed = [], []

    def pass_on(hop, q):
        for way in (0, 1):
            if hop > 0:
                along(way, hop - 1, q).wait_recv()
            if hop < half:
                sent.append(along(way, hop, q))
                sent[-1].start()
            if hop > 0 or way == 0:
                if pieces[q][0] < brink:
                    crossed.append(across(way, hop, q))
                    crossed[-1].start()
                crossed.append(share(way, hop, q))
                crossed[-1].start()

    early = [q for q, (at, size) in enumerate(pieces) if at + size <= pure]
    late = [q for q in range(len(pieces)) if q not in early]
    if spare:
        swap = pltpu.make_async_remote_copy(
            src_ref=packed_ref.at[pl.ds(wide, spare)],
            dst_ref=extra_ref,
            send_sem=es,
            recv_sem=er,
            device_id=twin,
            device_id_type=MESH,
        )
        swap.start()
    for q in early:
        pass_on(0, q)
    if spare:
        swap.wait_recv()

        def merge(i, carry):
            kept = packed_ref[wide - 1 - i]
            v_ref[s, base + wide - 1 - i] = jnp.where(i < pick_ref[1], extra_ref[i], kept)
            return carry

        lax.fori_loop(0, spare, merge, 0, unroll=8)
    for q in late:
        pass_on(0, q)
    table(m, brink, wide, full, (counts_in, offsets_in), (counts_ref, offsets_ref), ls, tab_ref)
    v_ref[s, pl.ds(base, pure)] = packed_ref[pl.ds(0, pure)]
    v_ref[:, brink] = jnp.zeros_like(v_ref[:, brink])
    for hop in range(1, half + 1):
        for q in range(len(pieces)):
            pass_on(hop, q)
    fetch.wait()
    for copy in crossed:
        copy.wait_recv()
    for copy in crossed + sent:
        copy.wait_send()
    if spare:
        swap.wait_send()


def expand_kernel(n, bands, tab_ref, v_ref, ranks_ref, out_ref, lhs_ref, sq_ref, out_buf, sems):
    s = lax.axis_index("section")
    share, tile = v_ref.shape[2:]
    mids = GROUP + 2 * W
    ends = GROUP + 4 * W
    groups = ranks_ref.shape[0] // GROUP
    empty = jnp.zeros((tile, tile), v_ref.dtype)

    def put(group, a):
        half = lax.rem(group, 2)
        return pltpu.make_async_copy(out_buf.at[half, a], out_ref.at[group * GROUP + a], sems.at[half, a])

    def body(group, carry):
        def where(p, e):
            return tab_ref[0, (group * GROUP + p) * STRIDE + e + W]

        @pl.when(group >= 2)
        def reuse():
            for a in range(GROUP):
                put(group - 2, a).wait()

        for p in range(mids):
            for a in range(GROUP):
                d = p - W - a
                rows, cols = slice(a * share, (a + 1) * share), slice(p * tile, (p + 1) * tile)
                if abs(d) <= W:
                    lhs_ref[rows, cols] = v_ref[s, where(a + W, d)]
                else:
                    lhs_ref[rows, cols] = jnp.zeros((share, tile), lhs_ref.dtype)

        sums = [jnp.zeros((share, tile), jnp.float32) for _ in range(GROUP)]
        for b in range(0, ends, 2):
            lo, hi = max(0, b - 2 * W), min(mids, b + 2)
            sides = []
            for r in (b, b + 1):
                rows = []
                for p in range(lo, hi):
                    e = r - W - p
                    rows.append(v_ref[:, where(p, e)].reshape(tile, tile) if abs(e) <= W else empty)
                sides.append(jnp.concatenate(rows, axis=0))
            res = jnp.dot(
                lhs_ref[:, lo * tile : hi * tile],
                jnp.concatenate(sides, axis=1),
                preferred_element_type=jnp.float32,
            )
            for i in (0, 1):
                for a in range(GROUP):
                    o = b + i - a
                    if 0 <= o < bands:
                        value = res[a * share : (a + 1) * share, i * tile : (i + 1) * tile]
                        keep = ranks_ref[group * GROUP + a, o] < TOPK
                        squared = jnp.where(keep, value * value, jnp.float32(0.0))
                        sq_ref[a, o] = squared
                        sums[a] = sums[a] + squared
                    if o == bands - 1:
                        totals = jnp.sum(sums[a], axis=1, keepdims=True)
                        scaled = sq_ref[a] * (TOPK / (totals + 1e-6))[None]
                        out_buf[lax.rem(group, 2), a] = scaled.astype(out_buf.dtype)
        for a in range(GROUP):
            put(group, a).start()
        return carry

    lax.fori_loop(0, groups, body, 0)
    for group in range(max(0, groups - 2), groups):
        for a in range(GROUP):
            put(group, a).wait()


def shards(tiles, offsets, counts, ranks):
    panels, slots, share, tile = tiles.shape
    bands = ranks.shape[1]
    n = lax.axis_size("section")
    m = lax.axis_size("col")
    brink = W * slots
    full = panels * slots
    wides = [w for w in WIDES if full // 2 < w < full] + [full]
    scalars = pl.BlockSpec(memory_space=pltpu.SMEM)
    near = pl.BlockSpec(memory_space=pltpu.VMEM)
    far = pl.BlockSpec(memory_space=pltpu.HBM)

    fixed = [
        pltpu.with_memory_space_constraint(x, pltpu.HBM)
        for x in (counts, counts.reshape(-1, 128), tiles, counts.reshape(1, -1), offsets.T, ranks)
    ]
    packed, pick = pl.pallas_call(
        functools.partial(plan_kernel, m, wides),
        out_shape=(
            jax.ShapeDtypeStruct((full + slots, share, tile), tiles.dtype),
            jax.ShapeDtypeStruct((2,), jnp.int32),
        ),
        in_specs=[far] * 3,
        out_specs=(near, scalars),
        scratch_shapes=[
            pltpu.SMEM(counts.shape, jnp.int32),
            pltpu.VMEM((counts.size // 128, 128), jnp.int32),
            pltpu.VMEM(tiles.shape, tiles.dtype),
            pltpu.SemaphoreType.DMA((3,)),
        ],
        compiler_params=pltpu.CompilerParams(vmem_limit_bytes=8 << 20),
        name="plan",
    )(*fixed[:3])

    def level(wide):
        pure = 2 * wide - full
        pieces = cuts(sorted({0, pure, min(brink, wide), wide}), 80)
        count = len(pieces)
        edges = sum(1 for at, _ in pieces if at < brink)

        def run(packed, pick, counts, offsets, ranks):
            v, tab, ranks = pl.pallas_call(
                functools.partial(gather_kernel, n, m, brink, wide, full, pieces),
                out_shape=(
                    jax.ShapeDtypeStruct((n, brink + 1 + 2 * wide, share, tile), tiles.dtype),
                    jax.ShapeDtypeStruct((1, -(-(panels + 2 * W) * STRIDE // 128) * 128), jnp.int32),
                    jax.ShapeDtypeStruct(ranks.shape, ranks.dtype),
                ),
                in_specs=[near, scalars, far, far, far],
                out_specs=(near, near, near),
                scratch_shapes=[
                    pltpu.VMEM((max(full - wide, 1), share, tile), tiles.dtype),
                    pltpu.VMEM(counts.shape, counts.dtype),
                    pltpu.VMEM(offsets.shape, offsets.dtype),
                    pltpu.SemaphoreType.DMA((3,)),
                ]
                + [pltpu.SemaphoreType.DMA((2, n // 2, count))] * 2
                + [pltpu.SemaphoreType.DMA((n + 1, count))] * 2
                + [pltpu.SemaphoreType.DMA((n + 1, edges))] * 2
                + [pltpu.SemaphoreType.DMA] * 2,
                compiler_params=pltpu.CompilerParams(
                    collective_id=wides.index(wide), has_side_effects=True, vmem_limit_bytes=4 << 20
                ),
                name=f"gather{wide}",
            )(packed, pick, counts, offsets, ranks)
            return pl.pallas_call(
                functools.partial(expand_kernel, n, bands),
                out_shape=pltpu.HBM(ranks.shape, jnp.bfloat16),
                in_specs=[scalars, near, near],
                out_specs=far,
                scratch_shapes=[
                    pltpu.VMEM((GROUP * share, (GROUP + 2 * W) * tile), tiles.dtype),
                    pltpu.VMEM((GROUP, bands, share, tile), jnp.float32),
                    pltpu.VMEM((2, GROUP, bands, share, tile), jnp.bfloat16),
                    pltpu.SemaphoreType.DMA((2, GROUP)),
                ],
                compiler_params=pltpu.CompilerParams(vmem_limit_bytes=8 << 20),
                name=f"expand{wide}",
            )(tab, v, ranks)

        return run

    return lax.switch(pick[0], [level(wide) for wide in wides], packed, pick, *fixed[3:])


def solution(mesh):
    placed = (P("col", None, "section", None), P(), P(), P("col", None, "section", None))
    return jax.shard_map(
        shards,
        mesh=mesh,
        in_specs=placed,
        out_specs=P("col", None, "section", None),
        check_vma=False,
    )
```
